512 devices in a mesh: kvp: 64 (over z, y), tp: 8 (over x, core).
Axes of the slice: x: 4, y: 4, z: 16, core: 2. Of those that a mesh axis runs over, the one named last changes fastest.
Arguments:
- queries: bfloat16 [8, 8192], P(None, 'tp'), may hold values from -12 to 12
- key_pool: bfloat16 [2048, 64, 1024], P('kvp', None, 'tp'), may hold values from -5 to 5
- value_pool: bfloat16 [2048, 64, 1024], P('kvp', None, 'tp'), may hold values from -5 to 5
- block_table: int32 [64, 32], P('kvp'), may hold values from 0 to 31, each once within a row
- lengths: int32 [8], replicated, may hold values from 1 to 16384, 81920 in all
- residual_in: float32 [8, 8192], P(None, 'kvp'), may hold values from -12 to 12
- out_weight: bfloat16 [8192, 8192], P('tp', 'kvp'), may hold values from -0.0625 to 0.0625
- norm_gain: bfloat16 [8192], P('kvp'), may hold values from 0.25 to 1.75
- gate_weight: bfloat16 [8192, 28672], P('kvp', 'tp'), may hold values from -0.0625 to 0.0625
- up_weight: bfloat16 [8192, 28672], P('kvp', 'tp'), may hold values from -0.0625 to 0.0625
- down_weight: bfloat16 [28672, 8192], P('tp', 'kvp'), may hold values from -0.03125 to 0.03125
Outputs:
- attended: bfloat16 [8, 8192], P(None, 'tp')
- layer_out: float32 [8, 8192], P(None, 'kvp')
The draws below stay inside these ranges and needn't reach their ends.
Inputs may be any that keep to these rules, and one draw needn't show every extreme that they name: Row s is a permutation of 0 to 31; the page of request b's block j in KV shard s is s * 32 + block_table[s, b * 4 + j]. The lengths sum to 81920 and the longest is exactly 16384.
All inputs are finite; a program needn't handle non-finite values.
Results may differ from the reference program's by a relative error of at most 0.0056.
Values may be sent and summed in bfloat16 or wider, within the bound.
A program may use at most 64 MiB of HBM per device.

```python
import math
import jax
import jax.numpy as jnp
import numpy as np
from jax import lax

D = 8192
H = 64
KVH = 8
HD = 128
FF = 28672
BATCH = 8
PAGE = 64
SHARDS = 64
CTX = 16384
POOL_DEV = 32
PAGES = 2048


def draw_queries(key, part):
    shape = (BATCH, H * HD)
    drawn = jnp.clip(2.5 * jax.random.normal(jax.random.fold_in(key, 11), shape, jnp.float32), -12.0, 12.0)
    return drawn.astype(jnp.bfloat16)


def draw_key_pool(key, part):
    shape = (PAGES, PAGE, KVH * HD)
    drawn = jnp.clip(jax.random.normal(jax.random.fold_in(key, 13), shape, jnp.float32), -5.0, 5.0)
    return drawn.astype(jnp.bfloat16)


def draw_residual_in(key, part):
    width = D // SHARDS
    levels = jax.random.uniform(jax.random.fold_in(key, 31), (BATCH, SHARDS), jnp.float32, math.log(0.2), math.log(3.0))
    scales = jnp.repeat(jnp.exp(levels), width, axis=1)
    base = jnp.clip(jax.random.normal(jax.random.fold_in(key, 37), (BATCH, D), jnp.float32), -4.0, 4.0)
    return (base * scales).astype(jnp.float32)


def level_of(stream_key, shape, split, low, largest):
    level = 1.0
    for axis_at, parts in split:
        steps = jax.random.uniform(jax.random.fold_in(jax.random.fold_in(stream_key, 6), axis_at), (parts,), jnp.float32, low / len(split), largest / len(split))
        level = level * jnp.repeat(jnp.exp(steps), shape[axis_at] // parts).reshape((-1,) + (1,) * (len(shape) - 1 - axis_at))
    return level


def split_up(number_of, total, limit, lean):
    loads = [(1 << 20) // math.isqrt(grade ** lean) + 1 for grade in range(2, number_of + 1)]
    rest, holding = total - limit - (number_of - 1), [1] * (number_of - 1)
    while rest > 0:
        movable = [i for i in range(number_of - 1) if holding[i] < limit]
        whole, budget = sum([loads[i] for i in movable]), rest
        for i in movable:
            extra = min(limit - holding[i], max(1, budget * loads[i] // whole), rest)
            holding[i] = holding[i] + extra
            rest = rest - extra
    return np.array([limit] + holding)


def uneven_parts(rng, number_of, total, limit, skew):
    if number_of == 2:
        one = jax.random.randint(rng, (), max(1, total - limit), min(limit, total - 1) + 1)
        return jnp.stack([one, total - one])
    sizes = jnp.asarray(split_up(number_of, total, limit, skew), jnp.int32)
    pairs = (number_of - 1) // 2
    donor, receiver = sizes[1:1 + 2 * pairs:2], sizes[2:2 + 2 * pairs:2]
    slack = jnp.minimum(donor - 1, limit - receiver)
    shifted = jax.random.randint(jax.random.fold_in(rng, 1), (pairs,), 0, 1 << 20) % (slack + 1)
    sizes = sizes.at[1:1 + 2 * pairs:2].set(donor - shifted).at[2:2 + 2 * pairs:2].set(receiver + shifted)
    return sizes[jax.random.permutation(jax.random.fold_in(rng, 2), number_of)]


def centred(key, dims, scale, bound, shards=(), kind=jnp.bfloat16):
    gain = level_of(key, dims, shards, -0.22, 0.18) if shards else 1.0
    values = jax.random.normal(key, dims, jnp.float32) * scale * gain
    return jnp.minimum(jnp.maximum(values, -bound), bound).astype(kind)


def setup_inputs(seed: int = 0) -> dict:
    keys = jax.random.split(jax.random.key(seed), 12)
    return {
        "queries": draw_queries(jax.random.fold_in(keys[11], 71), 0),
        "key_pool": draw_key_pool(jax.random.fold_in(keys[11], 71), 0),
        "value_pool": centred(keys[2], (PAGES, PAGE, KVH * HD), 1.0, 5.0, ((0, 64), (2, 8))),
        "block_table": jax.vmap(lambda own: jax.random.permutation(own, POOL_DEV))(jax.random.split(keys[3], SHARDS)).reshape((SHARDS, POOL_DEV)).astype(jnp.int32),
        "lengths": uneven_parts(keys[4], BATCH, BATCH * CTX * 5 // 8, CTX, 1).astype(jnp.int32),
        "residual_in": draw_residual_in(jax.random.fold_in(keys[11], 71), 0),
        "out_weight": centred(keys[6], (H * HD, D), (H * HD) ** -0.5, 0.0625, ((0, 8), (1, 64))),
        "norm_gain": jnp.clip(1.0 + 0.15 * jax.random.normal(keys[7], (D,), jnp.float32), 0.25, 1.75).astype(jnp.bfloat16),
        "gate_weight": centred(keys[8], (D, FF), D ** -0.5, 0.0625, ((0, 64), (1, 8))),
        "up_weight": centred(keys[9], (D, FF), D ** -0.5, 0.0625, ((0, 64), (1, 8))),
        "down_weight": centred(keys[10], (FF, D), FF ** -0.5, 0.03125, ((0, 8), (1, 64))),
    }


def reference(queries, key_pool, value_pool, block_table, lengths, residual_in, out_weight, norm_gain, gate_weight, up_weight, down_weight):
    requests = queries.shape[0]
    shard_count = block_table.shape[0]
    pool_size = block_table.shape[1]
    blocks = pool_size // requests
    page_rows = key_pool.shape[1]
    context = shard_count * blocks * page_rows
    group_size = H // KVH
    offsets = (jnp.arange(shard_count, dtype=jnp.int32) * pool_size)[:, None]
    page_ids = (block_table.astype(jnp.int32) + offsets).reshape(shard_count, requests, blocks)
    page_ids = jnp.transpose(page_ids, (1, 0, 2))
    positions = jnp.arange(context, dtype=jnp.int32)

    def attend_request(request):
        wanted = page_ids[request].reshape(-1)
        key_rows = key_pool[wanted].reshape(context, KVH, HD).astype(jnp.float32)
        value_rows = value_pool[wanted].reshape(context, KVH, HD).astype(jnp.float32)
        query_heads = queries[request].reshape(KVH, group_size, HD).astype(jnp.float32)
        scores = jnp.einsum('kgd,tkd->kgt', query_heads, key_rows) * HD ** (-0.5)
        is_live = positions < lengths[request]
        masked = jnp.where(is_live, scores, -1e+30)
        row_peak = lax.optimization_barrier(jnp.max(masked, axis=-1, keepdims=True))
        weights = jnp.where(is_live, jnp.exp(masked - row_peak), 0.0)
        weight_sum = lax.optimization_barrier(jnp.sum(weights, axis=-1))
        rounded = lax.optimization_barrier(weights.astype(jnp.bfloat16)).astype(jnp.float32)
        out_sum = jnp.einsum('kgt,tkd->kgd', rounded, value_rows)
        return (out_sum / weight_sum[..., None]).reshape(H * HD)
    attended = lax.map(attend_request, jnp.arange(requests, dtype=jnp.int32)).astype(jnp.bfloat16)
    mixed = residual_in + jnp.dot(attended, out_weight, preferred_element_type=jnp.float32)
    inv_rms = lax.rsqrt(lax.optimization_barrier(jnp.sum(mixed * mixed, axis=1, keepdims=True)) / D + 0.1)
    normed = (mixed * inv_rms * norm_gain.astype(jnp.float32)).astype(jnp.bfloat16)
    gate_part = jnp.dot(normed, gate_weight, preferred_element_type=jnp.float32)
    up_part = jnp.dot(normed, up_weight, preferred_element_type=jnp.float32)
    hidden = (jax.nn.silu(gate_part) * up_part).astype(jnp.bfloat16)
    layer_out = mixed + jnp.dot(hidden, down_weight, preferred_element_type=jnp.float32)
    return (attended, layer_out)
```

```python
import jax
import jax.numpy as jnp
from jax import lax
from jax.experimental import pallas as pl
from jax.experimental.pallas import tpu as pltpu
from jax.sharding import PartitionSpec as P

MESH = pl.DeviceIdType.MESH
F32 = jnp.float32
BF16 = jnp.bfloat16

NY, NZ, NT = 4, 16, 8
B, HD = 8, 128
D = 8192
HL = 8
BLOCKS = 4
PAGE = 64
SPAN = BLOCKS * PAGE
TILES = 7
QUARTER = TILES * 128
UNITS = 2 * TILES
FAR_FIRST = (8, 7, 9, 6, 10, 5, 11, 4, 12, 3, 13, 2, 14, 1, 15)


def iota(shape, dim):
    return lax.broadcasted_iota(jnp.int32, shape, dim)


def kernel(
    q_h, k_h, v_h, tab_h, len_h, res_h, wo_h, gain_h, wg_h, wu_h, wd_h,
    att_h, lay_h,
    q_v, k_v, v_v, tab_s, len_s, res_v, wo_v, gain_v, wg_v, wu_v, wd_v,
    osend, stsend, yo, yst, zo, zst, attb, attv, tp1, sqy, sqz, sqsend,
    ysend, yrecv, units, zrecv, hidz, yh, tp2, layv,
    lsem, osem, yo_s, yo_r, yst_s, yst_r, zo_s, zo_r, zst_s, zst_r, ya_s, ya_r,
    t1_s, t1_r, sy_s, sy_r, sz_s, sz_r, yr_s, yr_r, zr_s, zr_r, za_s, za_r,
    yh_s, yh_r, t2_s, t2_r,
):
    kv = lax.axis_index("kvp")
    tp = lax.axis_index("tp")
    z = lax.div(kv, NY)
    y = lax.rem(kv, NY)

    def ypos(d):
        return lax.rem(y + d, NY)

    def zpos(d):
        return lax.rem(z + d, NZ)

    def ydev(d):
        return (z * NY + ypos(d), tp)

    def zdev(d):
        return (zpos(d) * NY + y, tp)

    def tdev(d):
        return (kv, lax.rem(tp + d, NT))

    barrier = pltpu.get_barrier_semaphore()
    partners = (
        [zdev(d) for d in FAR_FIRST]
        + [tdev(d) for d in range(1, NT)]
        + [ydev(d) for d in range(1, NY)]
    )
    for dev in partners:
        pl.semaphore_signal(barrier, inc=1, device_id=dev, device_id_type=MESH)

    loads = []

    def load(src, dst):
        copy = pltpu.make_async_copy(src, dst, lsem.at[len(loads)])
        copy.start()
        loads.append(copy)
        return copy

    l_tab = load(tab_h, tab_s)
    l_len = load(len_h, len_s)
    l_q = load(q_h, q_v)
    l_k = [load(k_h.at[pl.ds(8 * i, 8)], k_v.at[pl.ds(8 * i, 8)]) for i in range(4)]
    l_v = [load(v_h.at[pl.ds(8 * i, 8)], v_v.at[pl.ds(8 * i, 8)]) for i in range(4)]
    l_res = load(res_h, res_v)
    l_gain = load(gain_h, gain_v)
    l_wo = load(wo_h, wo_v)
    l_w = []
    for d in range(NY):
        cols = pl.ds(pl.multiple_of(ypos(d) * QUARTER, 128), QUARTER)
        l_w.append((load(wg_h.at[:, cols], wg_v.at[d]), load(wu_h.at[:, cols], wu_v.at[d])))
    l_wd = []
    for d in range(NY):
        rows = pl.ds(pl.multiple_of(ypos(d) * QUARTER, 128), QUARTER)
        l_wd.append(load(wd_h.at[rows, :], wd_v.at[d]))

    sent = []

    def send(src, dst, ssem, rsem, dev):
        copy = pltpu.make_async_remote_copy(
            src_ref=src, dst_ref=dst, send_sem=ssem, recv_sem=rsem, device_id=dev, device_id_type=MESH
        )
        copy.start()
        return copy

    def arrived(dst, ssem, rsem, dev):
        pltpu.make_async_remote_copy(
            src_ref=dst, dst_ref=dst, send_sem=ssem, recv_sem=rsem, device_id=dev, device_id_type=MESH
        ).wait_recv()

    def left(copies):
        for copy in copies:
            copy.wait_send()

    l_tab.wait()
    l_len.wait()
    l_q.wait()
    qf = q_v[...].astype(F32)
    q_rows = jnp.concatenate([qf[:, h * HD : (h + 1) * HD] for h in range(HL)], axis=0).astype(BF16)
    request = iota((HL * B, SPAN), 0) & (B - 1)
    position = iota((HL * B, SPAN), 1) + kv * SPAN
    length = jnp.full((HL * B, SPAN), len_s[0], jnp.int32)
    for b in range(1, B):
        length = jnp.where(request == b, len_s[b], length)
    live = position < length
    for copy in l_k:
        copy.wait()
    scores = None
    for b in range(B):
        keys = jnp.concatenate([k_v[tab_s[0, b * BLOCKS + j]] for j in range(BLOCKS)], axis=0)
        part = lax.dot_general(q_rows, keys, (((1,), (1,)), ((), ())), preferred_element_type=F32)
        scores = part if scores is None else jnp.where(request == b, part, scores)
    masked = jnp.where(live, scores * HD ** (-0.5), -1e30)
    peak = jnp.max(masked, axis=1, keepdims=True)
    weights = jnp.where(live, jnp.exp(masked - peak), 0.0)
    total = jnp.sum(weights, axis=1, keepdims=True)
    for copy in l_v:
        copy.wait()
    out = None
    for b in range(B):
        values = jnp.concatenate([v_v[tab_s[0, b * BLOCKS + j]] for j in range(BLOCKS)], axis=0)
        mine = jnp.where(request == b, weights, 0.0).astype(BF16)
        part = jnp.dot(mine, values, preferred_element_type=F32)
        out = part if out is None else out + part
    out = out.astype(BF16).reshape(NY, 2, B, HD)

    row16 = iota((16, 128), 0)
    lane16 = iota((16, 128), 1)
    diag = row16 == lane16
    diag_up = row16 + 16 == lane16
    osend[...] = out
    for j in range(NY):
        rows = slice(16 * j, 16 * j + 16)
        spread = jnp.where(diag, peak[rows], 0.0) + jnp.where(diag_up, total[rows], 0.0)
        stsend[j] = jnp.sum(spread, axis=0, keepdims=True)

    pl.semaphore_wait(barrier, len(partners))

    copies = []
    for d in (2, 1, 3):
        j = ypos(d)
        copies.append(send(stsend.at[j], yst.at[NY - d], yst_s.at[d], yst_r.at[NY - d], ydev(d)))
        copies.append(send(osend.at[j], yo.at[NY - d], yo_s.at[d], yo_r.at[NY - d], ydev(d)))
    yo[0] = osend[y]
    yst[0] = stsend[y]
    for k in range(1, NY):
        arrived(yst.at[k], yst_s.at[k], yst_r.at[k], ydev(k))
        arrived(yo.at[k], yo_s.at[k], yo_r.at[k], ydev(k))

    def as_column(line):
        return jnp.sum(jnp.where(diag, line, 0.0), axis=1, keepdims=True)

    stats = jnp.concatenate([yst[k] for k in range(NY)], axis=0)
    peak = jnp.max(stats, axis=0, keepdims=True)
    factor = jnp.exp(stats - peak)
    total = jnp.sum(factor * pltpu.roll(stats, 112, 1), axis=0, keepdims=True)
    mixed_out = None
    for k in range(NY):
        part = as_column(factor[k : k + 1]) * yo[k].astype(F32).reshape(16, HD)
        mixed_out = part if mixed_out is None else mixed_out + part
    lane1 = iota((1, 128), 1)
    zo[z] = mixed_out.astype(BF16).reshape(2, B, HD)
    zst[z] = jnp.where(lane1 < 16, peak, jnp.where(lane1 < 32, pltpu.roll(total, 16, 1), 0.0))

    zcopies = []
    for d in FAR_FIRST:
        zcopies.append(send(zst.at[z], zst.at[z], zst_s.at[d], zst_r.at[NZ - d], zdev(d)))
        zcopies.append(send(zo.at[z], zo.at[z], zo_s.at[d], zo_r.at[NZ - d], zdev(d)))
    left(copies)
    for d in range(1, NZ):
        arrived(zst.at[zpos(d)], zst_s.at[d], zst_r.at[d], zdev(d))
    stats = jnp.concatenate([zst[k] for k in range(NZ)], axis=0)
    peak = jnp.max(stats, axis=0, keepdims=True)
    factor = jnp.exp(stats - peak)
    total = jnp.sum(factor * pltpu.roll(stats, 112, 1), axis=0, keepdims=True)
    share = factor / total
    columns = [as_column(share[k : k + 1]) for k in range(NZ)]
    for d in range(1, NZ):
        arrived(zo.at[zpos(d)], zo_s.at[d], zo_r.at[d], zdev(d))
    att = None
    for k in range(NZ):
        part = columns[k] * zo[k].astype(F32).reshape(16, HD)
        att = part if att is None else att + part
    pair = pl.ds(2 * y, 2)
    attb[pair] = att.astype(BF16).reshape(2, B, HD)

    copies = [send(attb.at[pair], attb.at[pair], ya_s.at[d], ya_r.at[NY - d], ydev(d)) for d in (2, 1, 3)]
    left(zcopies)
    l_wo.wait()
    for k in range(1, NY):
        theirs = pl.ds(2 * ypos(k), 2)
        arrived(attb.at[theirs], ya_s.at[k], ya_r.at[k], ydev(k))
    for h in range(HL):
        attv[:, h * HD : (h + 1) * HD] = attb[h]

    tp1[tp] = jnp.dot(attv[...], wo_v[...], preferred_element_type=F32)
    tcopies = [
        send(tp1.at[tp], tp1.at[tp], t1_s.at[d], t1_r.at[NT - d], tdev(d)) for d in (4, 5, 3, 2, 6, 7, 1)
    ]
    att_copy = pltpu.make_async_copy(attv, att_h, osem.at[0])
    att_copy.start()
    left(copies)
    l_res.wait()
    l_gain.wait()
    for k in range(1, NT):
        arrived(tp1.at[lax.rem(tp + k, NT)], t1_s.at[k], t1_r.at[k], tdev(k))
    shared = tp1[0]
    for k in range(1, NT):
        shared = shared + tp1[k]
    mixed = res_v[...] + shared

    row8 = iota((B, 128), 0)
    lane8 = iota((B, 128), 1)
    squares = jnp.sum(mixed * mixed, axis=1, keepdims=True)
    sqy[0] = jnp.sum(jnp.where(row8 == lane8, squares, 0.0), axis=0, keepdims=True)
    scaled = (mixed * gain_v[...].astype(F32)).astype(BF16)
    copies = [send(sqy.at[0], sqy.at[NY - d], sy_s.at[d], sy_r.at[NY - d], ydev(d)) for d in (2, 1, 3)]

    def gate_up(d):
        l_w[d][0].wait()
        l_w[d][1].wait()
        gate = jnp.dot(scaled, wg_v[d], preferred_element_type=F32)
        up = jnp.dot(scaled, wu_v[d], preferred_element_type=F32)
        return [a[:, t * 128 : (t + 1) * 128] for a in (gate, up) for t in range(TILES)]

    for d in (2, 1, 3):
        parts = gate_up(d)
        for i in range(2 * TILES):
            ysend[d, i] = parts[i].astype(BF16)
        copies.append(send(ysend.at[d], yrecv.at[NY - d], yr_s.at[d], yr_r.at[NY - d], ydev(d)))
    parts = gate_up(0)
    for k in range(1, NY):
        arrived(sqy.at[k], sy_s.at[k], sy_r.at[k], ydev(k))
    sqz[0] = (sqy[0] + sqy[1]) + (sqy[2] + sqy[3])
    for d in FAR_FIRST:

        @pl.when(zpos(d) < UNITS)
        def _():
            send(sqz.at[0], sqz.at[NZ - d], sz_s.at[d], sz_r.at[NZ - d], zdev(d))

    left(tcopies)
    for k in range(1, NY):
        arrived(yrecv.at[k], yr_s.at[k], yr_r.at[k], ydev(k))
        for i in range(2 * TILES):
            parts[i] = parts[i] + yrecv[k, i].astype(F32)
    low = row8 < 4
    for t in range(TILES):
        gate, up = parts[t], parts[TILES + t]
        units[2 * t] = jnp.where(low, gate, pltpu.roll(up, 4, 0)).astype(BF16)
        units[2 * t + 1] = jnp.where(low, pltpu.roll(gate, 4, 0), up).astype(BF16)

    for d in FAR_FIRST:

        @pl.when(zpos(d) < UNITS)
        def _():
            send(units.at[zpos(d)], zrecv.at[NZ - d], zr_s.at[d], zr_r.at[NZ - d], zdev(d))

    left(copies)

    @pl.when(z < UNITS)
    def _():
        half = lax.rem(z, 2)
        for k in range(1, NZ):
            arrived(sqz.at[k], sz_s.at[k], sz_r.at[k], zdev(k))
        squares = sqz[0]
        for k in range(1, NZ):
            squares = squares + sqz[k]
        wanted = lane8 == (row8 & 3) + 4 * half
        column = jnp.sum(jnp.where(wanted, squares, 0.0), axis=1, keepdims=True)
        inv_rms = lax.rsqrt(column / D + 0.1)
        own = units[z].astype(F32)
        for k in range(1, NZ):
            arrived(zrecv.at[k], zr_s.at[k], zr_r.at[k], zdev(k))
            own = own + zrecv[k].astype(F32)
        own = own * inv_rms
        hidden = own / (1.0 + jnp.exp(-own)) * pltpu.roll(own, 4, 0)
        placed = jnp.where(half == 0, hidden, pltpu.roll(hidden, 4, 0))
        mine = lax.shift_right_logical(row8, 2) == half
        hidz[z] = jnp.where(mine, placed, 0.0).astype(BF16)
        for d in FAR_FIRST:
            send(hidz.at[z], hidz.at[z], za_s.at[d], za_r.at[NZ - d], zdev(d))

    for d in range(1, NZ):

        @pl.when(zpos(d) < UNITS)
        def _():
            arrived(hidz.at[zpos(d)], za_s.at[d], za_r.at[d], zdev(d))

    for t in range(TILES):
        yh[0, t] = hidz[2 * t] + hidz[2 * t + 1]
    copies = [send(yh.at[0], yh.at[NY - d], yh_s.at[d], yh_r.at[NY - d], ydev(d)) for d in (2, 1, 3)]

    def down(k):
        l_wd[k].wait()
        rows = jnp.concatenate([yh[k, t] for t in range(TILES)], axis=1)
        return jnp.dot(rows, wd_v[k], preferred_element_type=F32)

    part = down(0)
    for k in (1, 3, 2):
        arrived(yh.at[k], yh_s.at[k], yh_r.at[k], ydev(k))
        part = part + down(k)
    tp2[tp] = part
    tcopies = [
        send(tp2.at[tp], tp2.at[tp], t2_s.at[d], t2_r.at[NT - d], tdev(d)) for d in (4, 5, 3, 2, 6, 7, 1)
    ]
    left(copies)
    for d in range(1, NZ):

        @pl.when(zpos(d) < UNITS)
        def _():
            pltpu.make_async_remote_copy(
                sqz.at[0], sqz.at[0], sz_s.at[d], sz_r.at[d], zdev(d), MESH
            ).wait_send()
            pltpu.make_async_remote_copy(
                units.at[0], units.at[0], zr_s.at[d], zr_r.at[d], zdev(d), MESH
            ).wait_send()

    @pl.when(z < UNITS)
    def _():
        for d in range(1, NZ):
            pltpu.make_async_remote_copy(
                hidz.at[0], hidz.at[0], za_s.at[d], za_r.at[d], zdev(d), MESH
            ).wait_send()

    att_copy.wait()
    for k in range(1, NT):
        arrived(tp2.at[lax.rem(tp + k, NT)], t2_s.at[k], t2_r.at[k], tdev(k))
    shared = tp2[0]
    for k in range(1, NT):
        shared = shared + tp2[k]
    layv[...] = mixed + shared
    lay_copy = pltpu.make_async_copy(layv, lay_h, osem.at[1])
    lay_copy.start()
    left(tcopies)
    lay_copy.wait()


def body(queries, key_pool, value_pool, block_table, lengths, residual_in, out_weight, norm_gain,
         gate_weight, up_weight, down_weight):
    vm = pltpu.VMEM
    dma = pltpu.SemaphoreType.DMA
    scratch = [
        vm((B, HL * HD), BF16), vm((32, PAGE, HD), BF16), vm((32, PAGE, HD), BF16),
        pltpu.SMEM((1, 32), jnp.int32), pltpu.SMEM((B,), jnp.int32), vm((B, 128), F32),
        vm((HL * HD, 128), BF16), vm((1, 128), BF16),
        vm((NY, 128, QUARTER), BF16), vm((NY, 128, QUARTER), BF16), vm((NY, QUARTER, 128), BF16),
        vm((NY, 2, B, HD), BF16), vm((NY, 1, 128), F32),
        vm((NY, 2, B, HD), BF16), vm((NY, 1, 128), F32),
        vm((NZ, 2, B, HD), BF16), vm((NZ, 1, 128), F32),
        vm((HL, B, HD), BF16), vm((B, HL * HD), BF16), vm((NT, B, 128), F32),
        vm((NY, 1, 128), F32), vm((NZ, 1, 128), F32), vm((1, 128), F32),
        vm((NY, 2 * TILES, B, 128), BF16), vm((NY, 2 * TILES, B, 128), BF16),
        vm((NZ, B, 128), BF16), vm((NZ, B, 128), BF16), vm((UNITS, B, 128), BF16),
        vm((NY, TILES, B, 128), BF16), vm((NT, B, 128), F32), vm((B, 128), F32),
        dma((32,)), dma((2,)),
        dma((NY,)), dma((NY,)), dma((NY,)), dma((NY,)),
        dma((NZ,)), dma((NZ,)), dma((NZ,)), dma((NZ,)),
        dma((NY,)), dma((NY,)), dma((NT,)), dma((NT,)),
        dma((NY,)), dma((NY,)), dma((NZ,)), dma((NZ,)),
        dma((NY,)), dma((NY,)), dma((NZ,)), dma((NZ,)),
        dma((NZ,)), dma((NZ,)), dma((NY,)), dma((NY,)), dma((NT,)), dma((NT,)),
    ]
    anywhere = pl.BlockSpec(memory_space=pl.ANY)
    return pl.pallas_call(
        kernel,
        out_shape=(
            jax.ShapeDtypeStruct((B, HL * HD), BF16),
            jax.ShapeDtypeStruct((B, 128), F32),
        ),
        in_specs=[anywhere] * 11,
        out_specs=(anywhere, anywhere),
        scratch_shapes=scratch,
        compiler_params=pltpu.CompilerParams(collective_id=0, has_side_effects=True),
        name="layer",
    )(queries, key_pool, value_pool, block_table, lengths, residual_in, out_weight,
      norm_gain.reshape(1, 128), gate_weight, up_weight, down_weight)


def solution(mesh):
    placed = (
        P(None, "tp"), P("kvp", None, "tp"), P("kvp", None, "tp"), P("kvp", None), P(),
        P(None, "kvp"), P("tp", "kvp"), P("kvp"), P("kvp", "tp"), P("kvp", "tp"), P("tp", "kvp"),
    )
    return jax.shard_map(
        body, mesh=mesh, in_specs=placed, out_specs=(P(None, "tp"), P(None, "kvp")), check_vma=False
    )
```
